32 devices in a mesh: rows: 32 (over z, y, x, core).
Axes of the slice: x: 2, y: 2, z: 4, core: 2. Of those that a mesh axis runs over, the one named last changes fastest.
Arguments:
- history: float32 [32, 512, 4096], P(None, 'rows'), may hold values from 0.2 to 1.8, as said below
- source: float32 [512, 4096], P('rows'), may hold values from 0.5 to 2, as said below
- diffusivity: float32 [512, 4096], P('rows'), may hold values from 0.5 to 2, as said below
- target: float32 [512, 4096], P('rows'), may hold values from -0.5 to 2.5, as said below
Outputs:
- update: float32 [512, 4096], P('rows')
- totals: float32 [2], replicated
The draws below stay inside these ranges and needn't reach their ends.
Inputs may be any that keep to these rules, and one draw needn't show every extreme that they name: `history`: every level is a field between 0.2 and 1.8, smooth with a small cell-by-cell variation. `source`: a positive field between 0.5 and 2. `diffusivity`: a positive field between 0.5 and 2, smooth with a small cell-by-cell variation. `target`: a field between -0.5 and 2.5, smooth with a small cell-by-cell variation.
All inputs are finite; a program needn't handle non-finite values.
Results may differ from the reference program's by a relative error of at most 0.0003.
Values sent between devices are 32-bit elements; how exact they have to be, the bound alone decides.
A program may use at most 128 MiB of HBM per device.

```python
import math
import jax
import jax.numpy as jnp
from jax import lax

NY = 4096
LEVELS = 32
STIFF = 1024
NX = 512


def smooth_pattern(base_key, row_count, col_count):
    subkeys = jax.random.split(base_key, 6)
    mode_count = 8
    two_pi = 2.0 * math.pi
    freq_rows = jax.random.uniform(subkeys[0], (mode_count,), jnp.float32, 0.5, 3.0)
    freq_cols = jax.random.uniform(subkeys[1], (mode_count,), jnp.float32, 0.5, 3.0)
    phase_rows = jax.random.uniform(subkeys[2], (mode_count,), jnp.float32, 0.0, two_pi)
    phase_cols = jax.random.uniform(subkeys[3], (mode_count,), jnp.float32, 0.0, two_pi)
    amplitude = 0.6 * jax.random.normal(subkeys[4], (mode_count,), jnp.float32)
    pos_rows = jnp.arange(row_count, dtype=jnp.float32) / row_count
    pos_cols = jnp.arange(col_count, dtype=jnp.float32) / col_count
    wave_rows = jnp.cos(two_pi * freq_rows[:, None] * pos_rows[None, :] + phase_rows[:, None])
    wave_cols = jnp.cos(two_pi * freq_cols[:, None] * pos_cols[None, :] + phase_cols[:, None])
    pattern = jnp.dot((amplitude[:, None] * wave_rows).T, wave_cols)
    jitter = 0.15 * jax.random.normal(subkeys[5], (row_count, col_count), jnp.float32)
    return jnp.tanh(pattern + jitter)


def banded_pattern(base_key, row_count, col_count):
    subkeys = jax.random.split(base_key, 6)
    two_pi = 2.0 * math.pi
    smooth_part = smooth_pattern(subkeys[0], row_count, col_count)
    column_noise = jax.random.uniform(subkeys[1], (col_count,), jnp.float32, -1.0, 1.0)
    row_noise = jax.random.uniform(subkeys[2], (row_count,), jnp.float32, -1.0, 1.0)
    phases = jax.random.uniform(subkeys[3], (2,), jnp.float32, 0.0, two_pi)
    pos_rows = jnp.arange(row_count, dtype=jnp.float32) / row_count
    pos_cols = jnp.arange(col_count, dtype=jnp.float32) / col_count
    column_mod = 0.75 + 0.25 * jnp.cos(two_pi * 1.5 * pos_rows + phases[0])
    row_mod = 0.75 + 0.25 * jnp.cos(two_pi * 1.5 * pos_cols + phases[1])
    jitter = 0.2 * jax.random.normal(subkeys[4], (row_count, col_count), jnp.float32)
    mixed = 0.5 * smooth_part + 1.3 * column_noise[None, :] * column_mod[:, None] + 1.3 * row_noise[:, None] * row_mod[None, :] + jitter
    return jnp.tanh(mixed)


def draw_history(key, part):
    level_keys = jax.random.split(jax.random.fold_in(key, 11), LEVELS)
    levels = lax.map(lambda one_key: smooth_pattern(one_key, NX, NY), level_keys)
    return 1.0 + 0.8 * levels


def draw_source(key, part):
    return 1.25 + 0.75 * banded_pattern(jax.random.fold_in(key, 23), NX, NY)


def draw_diffusivity(key, part):
    return jnp.exp(0.69 * smooth_pattern(jax.random.fold_in(key, 37), NX, NY))


def draw_target(key, part):
    return 1.0 + 1.5 * smooth_pattern(jax.random.fold_in(key, 41), NX, NY)


def setup_inputs(seed: int = 0) -> dict:
    arg_keys = jax.random.split(jax.random.key(seed), 5)
    return {
        "history": draw_history(jax.random.fold_in(arg_keys[4], 71), 0),
        "source": draw_source(jax.random.fold_in(arg_keys[4], 71), 0),
        "diffusivity": draw_diffusivity(jax.random.fold_in(arg_keys[4], 71), 0),
        "target": draw_target(jax.random.fold_in(arg_keys[4], 71), 0),
    }


frac_order = 0.6


def memory_weights(levels):
    moments = jnp.arange(levels + 1, dtype=jnp.float32)
    powered = moments ** (1.0 - frac_order)
    decay_terms = powered[1:] - powered[:-1]
    padding = jnp.zeros((1,), jnp.float32)
    return jnp.concatenate([decay_terms[1:], padding]) - jnp.concatenate([padding, decay_terms[1:]])


def line_bands(conduct):
    count_rows = conduct.shape[0]
    position = lax.broadcasted_iota(jnp.int32, conduct.shape, 0)
    coupling = -float(STIFF) * conduct
    sub_diag = jnp.where(position == 0, 0.0, coupling)
    sup_diag = jnp.where(position == count_rows - 1, 0.0, coupling)
    main_diag = 1.0 + 2.0 * float(STIFF) * conduct
    return sub_diag, main_diag, sup_diag


def thomas_solve(sub_diag, main_diag, sup_diag, right_side):
    def forward_pass(state_now, entries):
        ratio_prev, value_prev = state_now
        sub_now, main_now, sup_now, right_now = entries
        pivot_now = main_now - sub_now * ratio_prev
        ratio_new = sup_now / pivot_now
        value_new = (right_now - sub_now * value_prev) / pivot_now
        return (ratio_new, value_new), (ratio_new, value_new)

    zeros_row = jnp.zeros_like(right_side[0])
    _, (ratios, values_fwd) = lax.scan(forward_pass, (zeros_row, zeros_row), (sub_diag, main_diag, sup_diag, right_side))

    def backward_pass(later_value, entries):
        ratio_now, value_now = entries
        result_now = value_now - ratio_now * later_value
        return result_now, result_now

    _, solution = lax.scan(backward_pass, zeros_row, (ratios, values_fwd), reverse=True)
    return solution


def reference(history, source, diffusivity, target):
    weights = memory_weights(LEVELS)
    flat_hist = history.reshape(LEVELS, NX * NY)
    memory = jnp.dot(weights, flat_hist, precision=lax.Precision.HIGHEST).reshape(NX, NY)
    driven = history[0] - memory + source
    sub_x, main_x, sup_x = line_bands(diffusivity.T)
    swept = thomas_solve(sub_x, main_x, sup_x, driven.T).T
    sub_y, main_y, sup_y = line_bands(diffusivity)
    update = thomas_solve(sub_y, main_y, sup_y, swept)
    cell_count = float(NX * NY)
    totals = jnp.stack([jnp.sum(update) / cell_count, jnp.sum((update - target) ** 2) / cell_count])
    return update, totals
```

```python
import functools

import numpy as np
import jax
import jax.numpy as jnp
from jax import lax
from jax.experimental import pallas as pl
from jax.experimental.pallas import tpu as pltpu
from jax.sharding import PartitionSpec as P

STIFF = 1024
FRAC_ORDER = 0.6
LANES = 128
SUB = 8
CHUNK = 4


def driven_weights(levels):
    powered = np.arange(levels + 1, dtype=np.float64) ** (1.0 - FRAC_ORDER)
    decay = powered[1:] - powered[:-1]
    weights = np.append(decay[1:], 0.0) - np.append(0.0, decay[1:])
    combined = -weights
    combined[0] += 1.0
    return [float(w) for w in combined]


def rotate(x, shift, axis):
    size = x.shape[axis]
    shift = shift % size
    if shift == 0:
        return x
    unit = LANES if axis == 1 else SUB
    if shift % unit == 0:
        tail = lax.slice_in_dim(x, size - shift, size, axis=axis)
        head = lax.slice_in_dim(x, 0, size - shift, axis=axis)
        return jnp.concatenate([tail, head], axis)
    return pltpu.roll(x, shift, axis)


def pcr_level(lo, hi, excess, stride, axis):
    inv = 1.0 / (excess + lo + hi)
    g = lo * rotate(inv, stride, axis)
    h = hi * rotate(inv, -stride, axis)
    excess = excess + g * rotate(excess, stride, axis) + h * rotate(excess, -stride, axis)
    lo_new = g * rotate(lo, stride, axis)
    hi_new = h * rotate(hi, -stride, axis)
    return g, h, lo_new, hi_new, excess


def apply_level(d, g, h, stride, axis):
    return d + g * rotate(d, stride, axis) + h * rotate(d, -stride, axis)


def levels_of(length):
    return (length - 1).bit_length()


def kernel(nd, owners, weights, hist, src, dif, tgt, out, totals,
           hbuf, sbuf, dbuf, tbuf, acc, gx, hx, ivx, gy, hy, ivy, abuf, bbuf,
           s0, r0, s1, r1, s2, r2, xs, xr, tp, tr, gz, hz, ivz, send_sem, recv_sem, in_sem, h_sem):
    rows, width = dbuf.shape
    me = lax.axis_index("rows")
    spread = nd // owners
    nchunk = h_sem.shape[0]
    nlev_x, nlev_y, nlev_z = levels_of(width), levels_of(rows), levels_of(nd)
    stiff = float(STIFF)
    mine = me // spread

    load_dif = pltpu.make_async_copy(dif, dbuf, in_sem.at[0])
    load_dif.start()
    loads = []
    for c in range(nchunk):
        part = pl.ds(c * CHUNK, CHUNK)
        copy = pltpu.make_async_copy(hist.at[part], hbuf.at[part], h_sem.at[c])
        copy.start()
        loads.append(copy)
    load_src = pltpu.make_async_copy(src, sbuf, in_sem.at[1])
    load_src.start()
    load_tgt = pltpu.make_async_copy(tgt, tbuf, in_sem.at[2])
    load_tgt.start()

    barrier = pltpu.get_barrier_semaphore()

    @pl.loop(1, nd)
    def _(k):
        pl.semaphore_signal(barrier, inc=1, device_id=(lax.rem(me + k, nd),),
                            device_id_type=pl.DeviceIdType.MESH)

    def lane_part(o):
        return pl.ds(pl.multiple_of(o * LANES, LANES), LANES)

    is_owner = lax.rem(me, spread) == 0

    def when_owner(fn):
        if spread == 1:
            fn()
        else:
            pl.when(is_owner)(fn)

    def remote(src_ref, dst_ref, phase, dev):
        return pltpu.make_async_remote_copy(
            src_ref=src_ref, dst_ref=dst_ref, send_sem=send_sem.at[phase], recv_sem=recv_sem.at[phase],
            device_id=(dev,), device_id_type=pl.DeviceIdType.MESH)

    def scatter(s_ref, r_ref, phase):
        if spread == 1:
            @pl.loop(1, nd)
            def _(k):
                o = lax.rem(me + k, nd)
                remote(s_ref.at[:, lane_part(o)], r_ref.at[me], phase, o).start()
            r_ref[me] = s_ref[:, lane_part(me)]
        else:
            @pl.loop(0, owners)
            def _(o):
                @pl.when(o * spread != me)
                def _():
                    remote(s_ref.at[:, lane_part(o)], r_ref.at[me], phase, o * spread).start()

            @pl.when(is_owner)
            def _():
                r_ref[me] = s_ref[:, lane_part(mine)]

    def wait_all(ref, sem):
        pltpu.make_async_copy(ref, ref, sem).wait()

    def wait_gathered(r_ref, phase):
        wait_all(r_ref.at[pl.ds(0, nd - 1)], recv_sem.at[phase])

    def wait_from_owners(ref_of, phase):
        if spread == 1:
            wait_all(ref_of(owners - 1), recv_sem.at[phase])
        else:
            @pl.when(is_owner)
            def _():
                wait_all(ref_of(owners - 1), recv_sem.at[phase])

            @pl.when(jnp.logical_not(is_owner))
            def _():
                wait_all(ref_of(owners), recv_sem.at[phase])

    load_dif.wait()

    last = rows - 1
    pieces = 4
    piece = width // pieces

    def column_prep(i, carry):
        lanes = pl.ds(pl.multiple_of(i * piece, LANES), piece)
        inv_c = 1.0 / (stiff * dbuf[:, lanes])
        pos = lax.broadcasted_iota(jnp.int32, inv_c.shape, 0)
        is_last = pos == last
        zero, one = jnp.zeros_like(inv_c), jnp.ones_like(inv_c)
        lo = jnp.where((pos == 0) | is_last, zero, one)
        hi = jnp.where(pos >= last - 1, zero, one)
        excess = jnp.where(is_last, one, 2.0 + inv_c - lo - hi)
        inner = (pos > 0) & (pos < last - 1)
        excess = jnp.where(inner, inv_c, excess)
        a = jnp.where(pos == 0, one, zero)
        b = jnp.where(pos >= last - 1, one, zero)
        for k in range(nlev_y):
            g, h, lo, hi, excess = pcr_level(lo, hi, excess, 1 << k, 0)
            gy[k, :, lanes] = g
            hy[k, :, lanes] = h
            a = apply_level(a, g, h, 1 << k, 0)
            b = apply_level(b, g, h, 1 << k, 0)
        inv = 1.0 / (excess + lo + hi)
        ivy[:, lanes] = inv
        a, b = a * inv, b * inv
        abuf[:, lanes] = a
        bbuf[:, lanes] = b
        s0[0:1, lanes] = 2.0 + inv_c[last:last + 1] - b[last - 1:last]
        s0[1:2, lanes] = a[0:1]
        s0[2:3, lanes] = a[last - 1:last]
        s0[3:4, lanes] = jnp.sum(a * a, 0, keepdims=True)
        s0[4:5, lanes] = jnp.sum(a * b, 0, keepdims=True)
        s0[5:6, lanes] = jnp.sum(b * b, 0, keepdims=True)
        s0[6:7, lanes] = jnp.sum(a, 0, keepdims=True)
        s0[7:8, lanes] = jnp.sum(b, 0, keepdims=True)
        return carry

    lax.fori_loop(0, pieces, column_prep, 0)

    pl.semaphore_wait(barrier, nd - 1)
    scatter(s0, r0, 0)

    def row_prep(i, carry):
        part = pl.ds(pl.multiple_of(i * SUB, SUB), SUB)
        inv_c = 1.0 / (stiff * dbuf[part, :])
        pos = lax.broadcasted_iota(jnp.int32, inv_c.shape, 1)
        zero, one = jnp.zeros_like(inv_c), jnp.ones_like(inv_c)
        lo = jnp.where(pos == 0, zero, one)
        hi = jnp.where(pos == width - 1, zero, one)
        excess = jnp.where((pos == 0) | (pos == width - 1), inv_c + 1.0, inv_c)
        for k in range(nlev_x):
            g, h, lo, hi, excess = pcr_level(lo, hi, excess, 1 << k, 1)
            gx[k, part, :] = g
            hx[k, part, :] = h
        ivx[part, :] = 1.0 / (excess + lo + hi)
        return carry

    lax.fori_loop(0, rows // SUB, row_prep, 0)

    load_src.wait()
    for c in range(nchunk):
        loads[c].wait()
        base = sbuf if c == 0 else acc
        total = base[...]
        for k in range(c * CHUNK, (c + 1) * CHUNK):
            total = total + weights[k] * hbuf[k]
        acc[...] = total

    def row_solve(i, carry):
        part = pl.ds(pl.multiple_of(i * SUB, SUB), SUB)
        inv_c = 1.0 / (stiff * dbuf[part, :])
        d = acc[part, :] * inv_c
        for k in range(nlev_x):
            d = apply_level(d, gx[k, part, :], hx[k, part, :], 1 << k, 1)
        acc[part, :] = d * ivx[part, :] * inv_c
        return carry

    lax.fori_loop(0, rows // SUB, row_solve, 0)

    def column_solve(i, carry):
        lanes = pl.ds(pl.multiple_of(i * piece, LANES), piece)
        full = acc[:, lanes]
        pos = lax.broadcasted_iota(jnp.int32, full.shape, 0)
        d = jnp.where(pos == last, 0.0, full)
        for k in range(nlev_y):
            d = apply_level(d, gy[k, :, lanes], hy[k, :, lanes], 1 << k, 0)
        d = d * ivy[:, lanes]
        s1[0:1, lanes] = full[last:last + 1] + d[last - 1:last]
        s1[1:2, lanes] = d[0:1]
        acc[:, lanes] = d
        return carry

    lax.fori_loop(0, pieces, column_solve, 0)
    scatter(s1, r1, 1)

    load_tgt.wait()

    def error_parts(i, carry):
        lanes = pl.ds(pl.multiple_of(i * piece, LANES), piece)
        u = acc[:, lanes]
        gap = u - tbuf[:, lanes]
        s2[0:1, lanes] = jnp.sum(gap * abuf[:, lanes], 0, keepdims=True)
        s2[1:2, lanes] = jnp.sum(gap * bbuf[:, lanes], 0, keepdims=True)
        s2[2:3, lanes] = jnp.sum(gap * gap, 0, keepdims=True)
        s2[3:4, lanes] = jnp.sum(u, 0, keepdims=True)
        return carry

    lax.fori_loop(0, pieces, error_parts, 0)
    scatter(s2, r2, 2)

    def owner_work():
        wait_gathered(r0, 0)
        block = lax.broadcasted_iota(jnp.int32, (nd, LANES), 0)
        at_end = block == nd - 1

        def next_block(x):
            return jnp.where(at_end, 0.0, rotate(x, -1, 0))

        lo = jnp.where(block == 0, 0.0, r0[:, 2, :])
        hi = next_block(lo)
        excess = r0[:, 0, :] - next_block(r0[:, 1, :]) - lo - hi
        for k in range(nlev_z):
            g, h, lo, hi, excess = pcr_level(lo, hi, excess, 1 << k, 0)
            gz[k] = g
            hz[k] = h
        ivz[...] = 1.0 / (excess + lo + hi)
        wait_gathered(r1, 1)
        x = r1[:, 0, :] + next_block(r1[:, 1, :])
        for k in range(nlev_z):
            x = apply_level(x, gz[k], hz[k], 1 << k, 0)
        x = x * ivz[...]
        before = jnp.where(block == 0, 0.0, rotate(x, 1, 0))
        xs[:, 0, :] = before
        xs[:, 1, :] = x

        @pl.loop(1, nd)
        def _(k):
            dev = lax.rem(me + k, nd)
            remote(xs.at[dev], xr.at[:, lane_part(mine)], 3, dev).start()
        xr[:, lane_part(mine)] = xs[me]

        wait_gathered(r2, 2)
        mass = r2[:, 3, :] + r0[:, 6, :] * before + r0[:, 7, :] * x
        err = (r2[:, 2, :] + before * (2.0 * r2[:, 0, :] + r0[:, 3, :] * before + 2.0 * r0[:, 4, :] * x)
               + x * (2.0 * r2[:, 1, :] + r0[:, 5, :] * x))
        tp[0:1, :] = jnp.sum(mass, 0, keepdims=True)
        tp[1:2, :] = jnp.sum(err, 0, keepdims=True)

        @pl.loop(1, nd)
        def _(k):
            dev = lax.rem(me + k, nd)
            remote(tp, tr.at[mine], 4, dev).start()
        tr[mine] = tp[...]

    when_owner(owner_work)

    wait_from_owners(lambda n: xr.at[:, pl.ds(0, n * LANES)], 3)

    def finish(i, carry):
        lanes = pl.ds(pl.multiple_of(i * piece, LANES), piece)
        out[:, lanes] = (acc[:, lanes] + abuf[:, lanes] * xr[0:1, lanes] + bbuf[:, lanes] * xr[1:2, lanes])
        return carry

    lax.fori_loop(0, pieces, finish, 0)

    wait_from_owners(lambda n: tr.at[pl.ds(0, n)], 4)
    scale = 1.0 / float(nd * rows * width)
    totals[0] = jnp.sum(tr[:, 0, :]) * scale
    totals[1] = jnp.sum(tr[:, 1, :]) * scale

    def wait_sent(ref_of, phase):
        if spread == 1:
            wait_all(ref_of(owners - 1), send_sem.at[phase])
        else:
            @pl.when(is_owner)
            def _():
                wait_all(ref_of(owners - 1), send_sem.at[phase])

            @pl.when(jnp.logical_not(is_owner))
            def _():
                wait_all(ref_of(owners), send_sem.at[phase])

    for phase, ref in enumerate((s0, s1, s2)):
        wait_sent(lambda n, ref=ref: ref.at[:, pl.ds(0, n * LANES)], phase)

    def owner_sent():
        wait_all(xs.at[pl.ds(0, nd - 1)], send_sem.at[3])
        wait_all(xs.at[pl.ds(0, nd - 1)], send_sem.at[4])

    when_owner(owner_sent)


def solution(mesh):
    nd = mesh.shape["rows"]

    def body(history, source, diffusivity, target):
        levels, rows, width = history.shape
        owners = min(nd, width // LANES)
        f32 = jnp.float32
        vm = pltpu.VMEM
        nx, ny, nz = levels_of(width), levels_of(rows), levels_of(nd)
        field = vm((rows, width), f32)
        return pl.pallas_call(
            functools.partial(kernel, nd, owners, driven_weights(levels)),
            out_shape=(jax.ShapeDtypeStruct((rows, width), f32), jax.ShapeDtypeStruct((2,), f32)),
            in_specs=[pl.BlockSpec(memory_space=pl.ANY)] * 4,
            out_specs=(pl.BlockSpec(memory_space=pltpu.VMEM), pl.BlockSpec(memory_space=pltpu.SMEM)),
            scratch_shapes=[
                vm((levels, rows, width), f32), field, field, field, field,
                vm((nx, rows, width), f32), vm((nx, rows, width), f32), field,
                vm((ny, rows, width), f32), vm((ny, rows, width), f32), field, field, field,
                vm((8, width), f32), vm((nd, 8, LANES), f32),
                vm((2, width), f32), vm((nd, 2, LANES), f32),
                vm((4, width), f32), vm((nd, 4, LANES), f32),
                vm((nd, 2, LANES), f32), vm((2, width), f32),
                vm((2, LANES), f32), vm((owners, 2, LANES), f32),
                vm((nz, nd, LANES), f32), vm((nz, nd, LANES), f32), vm((nd, LANES), f32),
                pltpu.SemaphoreType.DMA((5,)), pltpu.SemaphoreType.DMA((5,)),
                pltpu.SemaphoreType.DMA((3,)), pltpu.SemaphoreType.DMA((levels // CHUNK,)),
            ],
            compiler_params=pltpu.CompilerParams(collective_id=0, has_side_effects=True),
        )(history, source, diffusivity, target)

    in_specs = (P(None, "rows", None), P("rows", None), P("rows", None), P("rows", None))
    return jax.shard_map(body, mesh=mesh, in_specs=in_specs, out_specs=(P("rows", None), P()), check_vma=False)
```

```python
import functools

import numpy as np
import jax
import jax.numpy as jnp
from jax import lax
from jax.experimental import pallas as pl
from jax.experimental.pallas import tpu as pltpu
from jax.sharding import PartitionSpec as P

STIFF = 1024
FRAC_ORDER = 0.6
LANES = 128
SUB = 8
CHUNK = 4


def driven_weights(levels):
    powered = np.arange(levels + 1, dtype=np.float64) ** (1.0 - FRAC_ORDER)
    decay = powered[1:] - powered[:-1]
    weights = np.append(decay[1:], 0.0) - np.append(0.0, decay[1:])
    combined = -weights
    combined[0] += 1.0
    return [float(w) for w in combined]


def rotate(x, shift, axis):
    size = x.shape[axis]
    shift = shift % size
    if shift == 0:
        return x
    unit = LANES if axis == 1 else SUB
    if shift % unit == 0:
        tail = lax.slice_in_dim(x, size - shift, size, axis=axis)
        head = lax.slice_in_dim(x, 0, size - shift, axis=axis)
        return jnp.concatenate([tail, head], axis)
    return pltpu.roll(x, shift, axis)


def pcr_level(lo, hi, excess, stride, axis):
    inv = 1.0 / (excess + lo + hi)
    g = lo * rotate(inv, stride, axis)
    h = hi * rotate(inv, -stride, axis)
    excess = excess + g * rotate(excess, stride, axis) + h * rotate(excess, -stride, axis)
    lo_new = g * rotate(lo, stride, axis)
    hi_new = h * rotate(hi, -stride, axis)
    return g, h, lo_new, hi_new, excess


def apply_level(d, g, h, stride, axis):
    return d + g * rotate(d, stride, axis) + h * rotate(d, -stride, axis)


def levels_of(length):
    return (length - 1).bit_length()


def kernel(nd, first, owners, spread, weights, hist, src, dif, tgt, free_out, a_out, b_out, xr, tr,
           hbuf, sbuf, dbuf, tbuf, acc, gx, hx, ivx, gy, hy, ivy, abuf, bbuf,
           s0, r0, s1, r1, s2, r2, xs, tp, gz, hz, ivz, send_sem, recv_sem, in_sem, h_sem):
    rows, width = dbuf.shape
    me = lax.axis_index("rows")
    cols = width // owners
    nchunk = h_sem.shape[0]
    nlev_x, nlev_y, nlev_z = levels_of(width), levels_of(rows), levels_of(nd)
    stiff = float(STIFF)
    mine = (me - first) // spread
    is_owner = (me >= first) & (me < first + owners * spread) & (lax.rem(me - first + nd, spread) == 0)

    load_dif = pltpu.make_async_copy(dif, dbuf, in_sem.at[0])
    load_dif.start()
    loads = []
    for c in range(nchunk):
        part = pl.ds(c * CHUNK, CHUNK)
        copy = pltpu.make_async_copy(hist.at[part], hbuf.at[part], h_sem.at[c])
        copy.start()
        loads.append(copy)
    load_src = pltpu.make_async_copy(src, sbuf, in_sem.at[1])
    load_src.start()
    load_tgt = pltpu.make_async_copy(tgt, tbuf, in_sem.at[2])
    load_tgt.start()

    barrier = pltpu.get_barrier_semaphore()

    def greet(dev):
        pl.semaphore_signal(barrier, inc=1, device_id=(dev,), device_id_type=pl.DeviceIdType.MESH)

    def to_others(fn):
        @pl.loop(1, nd)
        def _(k):
            fn(lax.rem(me + k, nd))

    def to_owners(fn):
        @pl.loop(0, owners)
        def _(o):
            dev = first + o * spread

            @pl.when(dev != me)
            def _():
                fn(dev, o)

    def by_role(owner_fn, other_fn):
        pl.when(is_owner)(owner_fn)
        pl.when(jnp.logical_not(is_owner))(other_fn)

    by_role(lambda: to_others(greet), lambda: to_owners(lambda dev, o: greet(dev)))

    def lane_part(o):
        return pl.ds(pl.multiple_of(o * cols, LANES), cols)

    def remote(src_ref, dst_ref, phase, dev):
        return pltpu.make_async_remote_copy(
            src_ref=src_ref, dst_ref=dst_ref, send_sem=send_sem.at[phase], recv_sem=recv_sem.at[phase],
            device_id=(dev,), device_id_type=pl.DeviceIdType.MESH)

    def scatter(s_ref, r_ref, phase):
        to_owners(lambda dev, o: remote(s_ref.at[:, lane_part(o)], r_ref.at[me], phase, dev).start())

        @pl.when(is_owner)
        def _():
            r_ref[me] = s_ref[:, lane_part(mine)]

    def wait_all(ref, sem):
        pltpu.make_async_copy(ref, ref, sem).wait()

    def wait_gathered(r_ref, phase):
        wait_all(r_ref.at[pl.ds(0, nd - 1)], recv_sem.at[phase])

    def wait_from_owners(ref_of, sem):
        by_role(lambda: wait_all(ref_of(owners - 1), sem), lambda: wait_all(ref_of(owners), sem))

    load_dif.wait()

    last = rows - 1
    pieces = 4
    piece = width // pieces

    def column_prep(i, carry):
        lanes = pl.ds(pl.multiple_of(i * piece, LANES), piece)
        inv_c = 1.0 / (stiff * dbuf[:, lanes])
        pos = lax.broadcasted_iota(jnp.int32, inv_c.shape, 0)
        is_last = pos == last
        zero, one = jnp.zeros_like(inv_c), jnp.ones_like(inv_c)
        lo = jnp.where((pos == 0) | is_last, zero, one)
        hi = jnp.where(pos >= last - 1, zero, one)
        excess = jnp.where(is_last, one, 2.0 + inv_c - lo - hi)
        inner = (pos > 0) & (pos < last - 1)
        excess = jnp.where(inner, inv_c, excess)
        a = jnp.where(pos == 0, one, zero)
        b = jnp.where(pos >= last - 1, one, zero)
        for k in range(nlev_y):
            g, h, lo, hi, excess = pcr_level(lo, hi, excess, 1 << k, 0)
            gy[k, :, lanes] = g
            hy[k, :, lanes] = h
            a = apply_level(a, g, h, 1 << k, 0)
            b = apply_level(b, g, h, 1 << k, 0)
        inv = 1.0 / (excess + lo + hi)
        ivy[:, lanes] = inv
        a, b = a * inv, b * inv
        abuf[:, lanes] = a
        bbuf[:, lanes] = b
        s0[0:1, lanes] = 2.0 + inv_c[last:last + 1] - b[last - 1:last]
        s0[1:2, lanes] = a[0:1]
        s0[2:3, lanes] = a[last - 1:last]
        s0[3:4, lanes] = jnp.sum(a * a, 0, keepdims=True)
        s0[4:5, lanes] = jnp.sum(a * b, 0, keepdims=True)
        s0[5:6, lanes] = jnp.sum(b * b, 0, keepdims=True)
        s0[6:7, lanes] = jnp.sum(a, 0, keepdims=True)
        s0[7:8, lanes] = jnp.sum(b, 0, keepdims=True)
        return carry

    lax.fori_loop(0, pieces, column_prep, 0)

    put_a = pltpu.make_async_copy(abuf, a_out, in_sem.at[3])
    put_b = pltpu.make_async_copy(bbuf, b_out, in_sem.at[4])
    put_a.start()
    put_b.start()

    def row_prep(i, carry):
        part = pl.ds(pl.multiple_of(i * SUB, SUB), SUB)
        inv_c = 1.0 / (stiff * dbuf[part, :])
        pos = lax.broadcasted_iota(jnp.int32, inv_c.shape, 1)
        zero, one = jnp.zeros_like(inv_c), jnp.ones_like(inv_c)
        lo = jnp.where(pos == 0, zero, one)
        hi = jnp.where(pos == width - 1, zero, one)
        excess = jnp.where((pos == 0) | (pos == width - 1), inv_c + 1.0, inv_c)
        for k in range(nlev_x):
            g, h, lo, hi, excess = pcr_level(lo, hi, excess, 1 << k, 1)
            gx[k, part, :] = g
            hx[k, part, :] = h
        ivx[part, :] = 1.0 / (excess + lo + hi)
        return carry

    lax.fori_loop(0, rows // SUB, row_prep, 0)

    by_role(lambda: pl.semaphore_wait(barrier, nd - 1), lambda: pl.semaphore_wait(barrier, owners))
    scatter(s0, r0, 0)

    load_src.wait()
    for c in range(nchunk):
        loads[c].wait()
        base = sbuf if c == 0 else acc
        total = base[...]
        for k in range(c * CHUNK, (c + 1) * CHUNK):
            total = total + weights[k] * hbuf[k]
        acc[...] = total

    def row_solve(i, carry):
        part = pl.ds(pl.multiple_of(i * SUB, SUB), SUB)
        inv_c = 1.0 / (stiff * dbuf[part, :])
        d = acc[part, :] * inv_c
        for k in range(nlev_x):
            d = apply_level(d, gx[k, part, :], hx[k, part, :], 1 << k, 1)
        acc[part, :] = d * ivx[part, :] * inv_c
        return carry

    lax.fori_loop(0, rows // SUB, row_solve, 0)

    def column_solve(i, carry):
        lanes = pl.ds(pl.multiple_of(i * piece, LANES), piece)
        full = acc[:, lanes]
        pos = lax.broadcasted_iota(jnp.int32, full.shape, 0)
        d = jnp.where(pos == last, 0.0, full)
        for k in range(nlev_y):
            d = apply_level(d, gy[k, :, lanes], hy[k, :, lanes], 1 << k, 0)
        d = d * ivy[:, lanes]
        s1[0:1, lanes] = full[last:last + 1] + d[last - 1:last]
        s1[1:2, lanes] = d[0:1]
        acc[:, lanes] = d
        return carry

    lax.fori_loop(0, pieces, column_solve, 0)
    scatter(s1, r1, 1)
    put_free = pltpu.make_async_copy(acc, free_out, in_sem.at[5])
    put_free.start()

    load_tgt.wait()

    def error_parts(i, carry):
        lanes = pl.ds(pl.multiple_of(i * piece, LANES), piece)
        u = acc[:, lanes]
        gap = u - tbuf[:, lanes]
        s2[0:1, lanes] = jnp.sum(gap * abuf[:, lanes], 0, keepdims=True)
        s2[1:2, lanes] = jnp.sum(gap * bbuf[:, lanes], 0, keepdims=True)
        s2[2:3, lanes] = jnp.sum(gap * gap, 0, keepdims=True)
        s2[3:4, lanes] = jnp.sum(u, 0, keepdims=True)
        return carry

    lax.fori_loop(0, pieces, error_parts, 0)
    scatter(s2, r2, 2)

    def owner_work():
        wait_gathered(r0, 0)
        block = lax.broadcasted_iota(jnp.int32, (nd, cols), 0)
        at_end = block == nd - 1

        def next_block(x):
            return jnp.where(at_end, 0.0, rotate(x, -1, 0))

        lo = jnp.where(block == 0, 0.0, r0[:, 2, :])
        hi = next_block(lo)
        excess = r0[:, 0, :] - next_block(r0[:, 1, :]) - lo - hi
        for k in range(nlev_z):
            g, h, lo, hi, excess = pcr_level(lo, hi, excess, 1 << k, 0)
            gz[k] = g
            hz[k] = h
        ivz[...] = 1.0 / (excess + lo + hi)
        wait_gathered(r1, 1)
        x = r1[:, 0, :] + next_block(r1[:, 1, :])
        for k in range(nlev_z):
            x = apply_level(x, gz[k], hz[k], 1 << k, 0)
        x = x * ivz[...]
        before = jnp.where(block == 0, 0.0, rotate(x, 1, 0))
        xs[:, 0, :] = before
        xs[:, 1, :] = x

        to_others(lambda dev: remote(xs.at[dev], xr.at[:, lane_part(mine)], 3, dev).start())
        xr[:, lane_part(mine)] = xs[me]

        wait_gathered(r2, 2)
        mass = r2[:, 3, :] + r0[:, 6, :] * before + r0[:, 7, :] * x
        err = (r2[:, 2, :] + before * (2.0 * r2[:, 0, :] + r0[:, 3, :] * before + 2.0 * r0[:, 4, :] * x)
               + x * (2.0 * r2[:, 1, :] + r0[:, 5, :] * x))
        tp[0:1, :] = jnp.sum(mass, 0, keepdims=True)
        tp[1:2, :] = jnp.sum(err, 0, keepdims=True)

        to_others(lambda dev: remote(tp, tr.at[mine], 4, dev).start())
        tr[mine] = tp[...]

    pl.when(is_owner)(owner_work)

    put_a.wait()
    put_b.wait()
    put_free.wait()
    for phase, ref in enumerate((s0, s1, s2)):
        wait_from_owners(lambda n, ref=ref: ref.at[:, pl.ds(0, n * cols)], send_sem.at[phase])
    wait_from_owners(lambda n: xr.at[:, pl.ds(0, n * cols)], recv_sem.at[3])
    wait_from_owners(lambda n: tr.at[pl.ds(0, n)], recv_sem.at[4])

    @pl.when(is_owner)
    def _():
        wait_all(xs.at[pl.ds(0, nd - 1)], send_sem.at[3])
        wait_all(xs.at[pl.ds(0, nd - 1)], send_sem.at[4])


def finish(cells, free, a, b, xr, tr, out, totals):
    out[...] = free[...] + a[...] * xr[0:1, :] + b[...] * xr[1:2, :]
    scale = 1.0 / float(cells)
    totals[0] = jnp.sum(tr[:, 0, :]) * scale
    totals[1] = jnp.sum(tr[:, 1, :]) * scale


def solution(mesh):
    nd = mesh.shape["rows"]

    def body(history, source, diffusivity, target):
        levels, rows, width = history.shape
        middle = max(nd // 2, 1)
        owners = min(middle, width // LANES)
        first, spread, cols = nd // 4, middle // owners, width // owners
        f32 = jnp.float32
        vm = pltpu.VMEM
        nx, ny, nz = levels_of(width), levels_of(rows), levels_of(nd)
        field = vm((rows, width), f32)
        whole = jax.ShapeDtypeStruct((rows, width), f32)
        in_hbm, in_vmem = pl.BlockSpec(memory_space=pl.ANY), pl.BlockSpec(memory_space=pltpu.VMEM)
        parts = pl.pallas_call(
            functools.partial(kernel, nd, first, owners, spread, driven_weights(levels)),
            out_shape=(whole, whole, whole, jax.ShapeDtypeStruct((2, width), f32),
                       jax.ShapeDtypeStruct((owners, 2, cols), f32)),
            in_specs=[in_hbm] * 4,
            out_specs=(in_hbm, in_hbm, in_hbm, in_vmem, in_vmem),
            scratch_shapes=[
                vm((levels, rows, width), f32), field, field, field, field,
                vm((nx, rows, width), f32), vm((nx, rows, width), f32), field,
                vm((ny, rows, width), f32), vm((ny, rows, width), f32), field, field, field,
                vm((8, width), f32), vm((nd, 8, cols), f32),
                vm((2, width), f32), vm((nd, 2, cols), f32),
                vm((4, width), f32), vm((nd, 4, cols), f32),
                vm((nd, 2, cols), f32), vm((2, cols), f32),
                vm((nz, nd, cols), f32), vm((nz, nd, cols), f32), vm((nd, cols), f32),
                pltpu.SemaphoreType.DMA((5,)), pltpu.SemaphoreType.DMA((5,)),
                pltpu.SemaphoreType.DMA((6,)), pltpu.SemaphoreType.DMA((levels // CHUNK,)),
            ],
            compiler_params=pltpu.CompilerParams(collective_id=0, has_side_effects=True),
        )(history, source, diffusivity, target)
        return pl.pallas_call(
            functools.partial(finish, nd * rows * width),
            out_shape=(whole, jax.ShapeDtypeStruct((2,), f32)),
            in_specs=[in_vmem] * 5,
            out_specs=(in_vmem, pl.BlockSpec(memory_space=pltpu.SMEM)),
        )(*parts)

    in_specs = (P(None, "rows", None), P("rows", None), P("rows", None), P("rows", None))
    return jax.shard_map(body, mesh=mesh, in_specs=in_specs, out_specs=(P("rows", None), P()), check_vma=False)
```

```python
import functools

import numpy as np
import jax
import jax.numpy as jnp
from jax import lax
from jax.experimental import pallas as pl
from jax.experimental.pallas import tpu as pltpu
from jax.sharding import PartitionSpec as P

STIFF = 1024
FRAC_ORDER = 0.6
LANES = 128
SUB = 8
CHUNK = 8
SUMMED = 4


def driven_weights(levels):
    powered = np.arange(levels + 1, dtype=np.float64) ** (1.0 - FRAC_ORDER)
    decay = powered[1:] - powered[:-1]
    weights = np.append(decay[1:], 0.0) - np.append(0.0, decay[1:])
    combined = -weights
    combined[0] += 1.0
    return [float(w) for w in combined]


def rotate(x, shift, axis):
    size = x.shape[axis]
    shift = shift % size
    if shift == 0:
        return x
    unit = LANES if axis == 1 else SUB
    if shift % unit == 0:
        tail = lax.slice_in_dim(x, size - shift, size, axis=axis)
        head = lax.slice_in_dim(x, 0, size - shift, axis=axis)
        return jnp.concatenate([tail, head], axis)
    return pltpu.roll(x, shift, axis)


def reciprocal(x):
    return 1.0 / x


def pcr_level(lo, hi, excess, stride, axis):
    inv = 1.0 / (excess + lo + hi)
    g = lo * rotate(inv, stride, axis)
    h = hi * rotate(inv, -stride, axis)
    excess = excess + g * rotate(excess, stride, axis) + h * rotate(excess, -stride, axis)
    lo_new = g * rotate(lo, stride, axis)
    hi_new = h * rotate(hi, -stride, axis)
    return g, h, lo_new, hi_new, excess


def pcr_main_level(lo, hi, main, stride, axis):
    inv = reciprocal(main)
    g = lo * rotate(inv, stride, axis)
    h = hi * rotate(inv, -stride, axis)
    main = main - g * lo - h * hi
    return g, h, g * rotate(lo, stride, axis), h * rotate(hi, -stride, axis), main


def apply_level(d, g, h, stride, axis):
    return d + g * rotate(d, stride, axis) + h * rotate(d, -stride, axis)


def levels_of(length):
    return (length - 1).bit_length()


def kernel(nd, first, owners, spread, weights, hist, src, dif, tgt, free_out, a_out, b_out, xr, tr,
           hbuf, sbuf, dbuf, tbuf, acc, gx, hx, ivx, gy, hy, ivy, abuf, bbuf,
           s0, r0, s1, r1, s2, r2, xs, tp, gz, hz, ivz, send_sem, recv_sem, in_sem, h_sem):
    rows, width = dbuf.shape
    me = lax.axis_index("rows")
    cols = width // owners
    nchunk = h_sem.shape[0]
    nlev_x, nlev_y, nlev_z = levels_of(width), levels_of(rows), levels_of(nd)
    stiff = float(STIFF)
    mine = (me - first) // spread
    is_owner = (me >= first) & (me < first + owners * spread) & (lax.rem(me - first + nd, spread) == 0)

    load_dif = pltpu.make_async_copy(dif, dbuf, in_sem.at[0])
    load_dif.start()
    loads = []
    for c in range(nchunk):
        part = pl.ds(c * CHUNK, CHUNK)
        copy = pltpu.make_async_copy(hist.at[part], hbuf.at[part], h_sem.at[c])
        copy.start()
        loads.append(copy)
    load_src = pltpu.make_async_copy(src, sbuf, in_sem.at[1])
    load_src.start()
    load_tgt = pltpu.make_async_copy(tgt, tbuf, in_sem.at[2])
    load_tgt.start()

    barrier = pltpu.get_barrier_semaphore()

    def greet(dev):
        pl.semaphore_signal(barrier, inc=1, device_id=(dev,), device_id_type=pl.DeviceIdType.MESH)

    def to_others(fn):
        @pl.loop(1, nd)
        def _(k):
            fn(lax.rem(me + k, nd))

    def to_owners(fn):
        @pl.loop(0, owners)
        def _(k):
            o = lax.rem(k + me, owners)
            dev = first + o * spread

            @pl.when(dev != me)
            def _():
                fn(dev, o)

    def by_role(owner_fn, other_fn):
        pl.when(is_owner)(owner_fn)
        pl.when(jnp.logical_not(is_owner))(other_fn)

    by_role(lambda: to_others(greet), lambda: to_owners(lambda dev, o: greet(dev)))

    def lane_part(o):
        return pl.ds(pl.multiple_of(o * cols, LANES), cols)

    def remote(src_ref, dst_ref, phase, dev):
        return pltpu.make_async_remote_copy(
            src_ref=src_ref, dst_ref=dst_ref, send_sem=send_sem.at[phase], recv_sem=recv_sem.at[phase],
            device_id=(dev,), device_id_type=pl.DeviceIdType.MESH)

    def scatter(s_ref, r_ref, phase):
        to_owners(lambda dev, o: remote(s_ref.at[:, lane_part(o)], r_ref.at[me], phase, dev).start())

        @pl.when(is_owner)
        def _():
            r_ref[me] = s_ref[:, lane_part(mine)]

    def wait_all(ref, sem):
        pltpu.make_async_copy(ref, ref, sem).wait()

    def wait_gathered(r_ref, phase):
        wait_all(r_ref.at[pl.ds(0, nd - 1)], recv_sem.at[phase])

    def wait_from_owners(ref_of, sem):
        by_role(lambda: wait_all(ref_of(owners - 1), sem), lambda: wait_all(ref_of(owners), sem))

    load_dif.wait()

    last = rows - 1
    pieces = 4
    piece = width // pieces

    def column_prep(i, carry):
        lanes = pl.ds(pl.multiple_of(i * piece, LANES), piece)
        inv_c = 1.0 / (stiff * dbuf[:, lanes])
        pos = lax.broadcasted_iota(jnp.int32, inv_c.shape, 0)
        is_last = pos == last
        zero, one = jnp.zeros_like(inv_c), jnp.ones_like(inv_c)
        lo = jnp.where((pos == 0) | is_last, zero, one)
        hi = jnp.where(pos >= last - 1, zero, one)
        excess = jnp.where(is_last, one, 2.0 + inv_c - lo - hi)
        inner = (pos > 0) & (pos < last - 1)
        excess = jnp.where(inner, inv_c, excess)
        a = jnp.where(pos == 0, one, zero)
        b = jnp.where(pos >= last - 1, one, zero)
        for k in range(nlev_y):
            g, h, lo, hi, excess = pcr_level(lo, hi, excess, 1 << k, 0)
            gy[k, :, lanes] = g
            hy[k, :, lanes] = h
            a = apply_level(a, g, h, 1 << k, 0)
            b = apply_level(b, g, h, 1 << k, 0)
        inv = 1.0 / (excess + lo + hi)
        ivy[:, lanes] = inv
        a, b = a * inv, b * inv
        abuf[:, lanes] = a
        bbuf[:, lanes] = b
        s0[0:1, lanes] = 2.0 + inv_c[last:last + 1] - b[last - 1:last]
        s0[1:2, lanes] = a[0:1]
        s0[2:3, lanes] = a[last - 1:last]
        s0[3:4, lanes] = jnp.sum(a * a, 0, keepdims=True)
        s0[4:5, lanes] = jnp.sum(a * b, 0, keepdims=True)
        s0[5:6, lanes] = jnp.sum(b * b, 0, keepdims=True)
        s0[6:7, lanes] = jnp.sum(a, 0, keepdims=True)
        s0[7:8, lanes] = jnp.sum(b, 0, keepdims=True)
        return carry

    lax.fori_loop(0, pieces, column_prep, 0)

    put_a = pltpu.make_async_copy(abuf, a_out, in_sem.at[3])
    put_b = pltpu.make_async_copy(bbuf, b_out, in_sem.at[4])
    put_a.start()
    put_b.start()

    by_role(lambda: pl.semaphore_wait(barrier, nd - 1), lambda: pl.semaphore_wait(barrier, owners))
    scatter(s0, r0, 0)

    def row_prep(i, carry):
        part = pl.ds(pl.multiple_of(i * SUB, SUB), SUB)
        inv_c = 1.0 / (stiff * dbuf[part, :])
        dbuf[part, :] = inv_c
        pos = lax.broadcasted_iota(jnp.int32, inv_c.shape, 1)
        zero, one = jnp.zeros_like(inv_c), jnp.ones_like(inv_c)
        lo = jnp.where(pos == 0, zero, one)
        hi = jnp.where(pos == width - 1, zero, one)
        excess = jnp.where((pos == 0) | (pos == width - 1), inv_c + 1.0, inv_c)
        for k in range(nlev_x):
            if k < SUMMED:
                g, h, lo, hi, excess = pcr_level(lo, hi, excess, 1 << k, 1)
                main = excess + lo + hi
            else:
                g, h, lo, hi, main = pcr_main_level(lo, hi, main, 1 << k, 1)
            gx[k, part, :] = g
            hx[k, part, :] = h
        ivx[part, :] = reciprocal(main)
        return carry

    lax.fori_loop(0, rows // SUB, row_prep, 0)

    load_src.wait()
    for c in range(nchunk):
        loads[c].wait()
        base = sbuf if c == 0 else acc

        def accumulate(i, carry):
            lanes = pl.ds(pl.multiple_of(i * piece, LANES), piece)
            total = base[:, lanes]
            for k in range(c * CHUNK, (c + 1) * CHUNK):
                total = total + weights[k] * hbuf[k, :, lanes]
            acc[:, lanes] = total
            return carry

        lax.fori_loop(0, pieces, accumulate, 0)

    def row_solve(i, carry):
        part = pl.ds(pl.multiple_of(i * SUB, SUB), SUB)
        inv_c = dbuf[part, :]
        d = acc[part, :] * inv_c
        for k in range(nlev_x):
            d = apply_level(d, gx[k, part, :], hx[k, part, :], 1 << k, 1)
        acc[part, :] = d * ivx[part, :] * inv_c
        return carry

    lax.fori_loop(0, rows // SUB, row_solve, 0)

    def column_solve(i, carry):
        lanes = pl.ds(pl.multiple_of(i * piece, LANES), piece)
        full = acc[:, lanes]
        pos = lax.broadcasted_iota(jnp.int32, full.shape, 0)
        d = jnp.where(pos == last, 0.0, full)
        for k in range(nlev_y):
            d = apply_level(d, gy[k, :, lanes], hy[k, :, lanes], 1 << k, 0)
        d = d * ivy[:, lanes]
        s1[0:1, lanes] = full[last:last + 1] + d[last - 1:last]
        s1[1:2, lanes] = d[0:1]
        acc[:, lanes] = d
        return carry

    lax.fori_loop(0, pieces, column_solve, 0)
    scatter(s1, r1, 1)
    put_free = pltpu.make_async_copy(acc, free_out, in_sem.at[5])
    put_free.start()

    load_tgt.wait()

    def error_parts(i, carry):
        lanes = pl.ds(pl.multiple_of(i * piece, LANES), piece)
        u = acc[:, lanes]
        gap = u - tbuf[:, lanes]
        s2[0:1, lanes] = jnp.sum(gap * abuf[:, lanes], 0, keepdims=True)
        s2[1:2, lanes] = jnp.sum(gap * bbuf[:, lanes], 0, keepdims=True)
        s2[2:3, lanes] = jnp.sum(gap * gap, 0, keepdims=True)
        s2[3:4, lanes] = jnp.sum(u, 0, keepdims=True)
        return carry

    lax.fori_loop(0, pieces, error_parts, 0)
    scatter(s2, r2, 2)

    def owner_work():
        wait_gathered(r0, 0)
        block = lax.broadcasted_iota(jnp.int32, (nd, cols), 0)
        at_end = block == nd - 1

        def next_block(x):
            return jnp.where(at_end, 0.0, rotate(x, -1, 0))

        lo = jnp.where(block == 0, 0.0, r0[:, 2, :])
        hi = next_block(lo)
        excess = r0[:, 0, :] - next_block(r0[:, 1, :]) - lo - hi
        for k in range(nlev_z):
            g, h, lo, hi, excess = pcr_level(lo, hi, excess, 1 << k, 0)
            gz[k] = g
            hz[k] = h
        ivz[...] = 1.0 / (excess + lo + hi)
        wait_gathered(r1, 1)
        x = r1[:, 0, :] + next_block(r1[:, 1, :])
        for k in range(nlev_z):
            x = apply_level(x, gz[k], hz[k], 1 << k, 0)
        x = x * ivz[...]
        before = jnp.where(block == 0, 0.0, rotate(x, 1, 0))
        xs[:, 0, :] = before
        xs[:, 1, :] = x

        to_others(lambda dev: remote(xs.at[dev], xr.at[:, lane_part(mine)], 3, dev).start())
        xr[:, lane_part(mine)] = xs[me]

        wait_gathered(r2, 2)
        mass = r2[:, 3, :] + r0[:, 6, :] * before + r0[:, 7, :] * x
        err = (r2[:, 2, :] + before * (2.0 * r2[:, 0, :] + r0[:, 3, :] * before + 2.0 * r0[:, 4, :] * x)
               + x * (2.0 * r2[:, 1, :] + r0[:, 5, :] * x))
        tp[0:1, :] = jnp.sum(mass, 0, keepdims=True)
        tp[1:2, :] = jnp.sum(err, 0, keepdims=True)

        to_others(lambda dev: remote(tp, tr.at[mine], 4, dev).start())
        tr[mine] = tp[...]

    pl.when(is_owner)(owner_work)

    put_a.wait()
    put_b.wait()
    put_free.wait()
    for phase, ref in enumerate((s0, s1, s2)):
        wait_from_owners(lambda n, ref=ref: ref.at[:, pl.ds(0, n * cols)], send_sem.at[phase])
    wait_from_owners(lambda n: xr.at[:, pl.ds(0, n * cols)], recv_sem.at[3])
    wait_from_owners(lambda n: tr.at[pl.ds(0, n)], recv_sem.at[4])

    @pl.when(is_owner)
    def _():
        wait_all(xs.at[pl.ds(0, nd - 1)], send_sem.at[3])
        wait_all(xs.at[pl.ds(0, nd - 1)], send_sem.at[4])


def finish(cells, free, a, b, xr, tr, out, totals):
    out[...] = free[...] + a[...] * xr[0:1, :] + b[...] * xr[1:2, :]
    scale = 1.0 / float(cells)
    totals[0] = jnp.sum(tr[:, 0, :]) * scale
    totals[1] = jnp.sum(tr[:, 1, :]) * scale


def solution(mesh):
    nd = mesh.shape["rows"]

    def body(history, source, diffusivity, target):
        levels, rows, width = history.shape
        middle = max(nd // 2, 1)
        owners = min(middle, width // LANES)
        first, spread, cols = nd // 4, middle // owners, width // owners
        f32 = jnp.float32
        vm = pltpu.VMEM
        nx, ny, nz = levels_of(width), levels_of(rows), levels_of(nd)
        field = vm((rows, width), f32)
        whole = jax.ShapeDtypeStruct((rows, width), f32)
        in_hbm, in_vmem = pl.BlockSpec(memory_space=pl.ANY), pl.BlockSpec(memory_space=pltpu.VMEM)
        parts = pl.pallas_call(
            functools.partial(kernel, nd, first, owners, spread, driven_weights(levels)),
            out_shape=(whole, whole, whole, jax.ShapeDtypeStruct((2, width), f32),
                       jax.ShapeDtypeStruct((owners, 2, cols), f32)),
            in_specs=[in_hbm] * 4,
            out_specs=(in_hbm, in_hbm, in_hbm, in_vmem, in_vmem),
            scratch_shapes=[
                vm((levels, rows, width), f32), field, field, field, field,
                vm((nx, rows, width), f32), vm((nx, rows, width), f32), field,
                vm((ny, rows, width), f32), vm((ny, rows, width), f32), field, field, field,
                vm((8, width), f32), vm((nd, 8, cols), f32),
                vm((2, width), f32), vm((nd, 2, cols), f32),
                vm((4, width), f32), vm((nd, 4, cols), f32),
                vm((nd, 2, cols), f32), vm((2, cols), f32),
                vm((nz, nd, cols), f32), vm((nz, nd, cols), f32), vm((nd, cols), f32),
                pltpu.SemaphoreType.DMA((5,)), pltpu.SemaphoreType.DMA((5,)),
                pltpu.SemaphoreType.DMA((6,)), pltpu.SemaphoreType.DMA((levels // CHUNK,)),
            ],
            compiler_params=pltpu.CompilerParams(collective_id=0, has_side_effects=True),
        )(history, source, diffusivity, target)
        return pl.pallas_call(
            functools.partial(finish, nd * rows * width),
            out_shape=(whole, jax.ShapeDtypeStruct((2,), f32)),
            in_specs=[in_vmem] * 5,
            out_specs=(in_vmem, pl.BlockSpec(memory_space=pltpu.SMEM)),
        )(*parts)

    in_specs = (P(None, "rows", None), P("rows", None), P("rows", None), P("rows", None))
    return jax.shard_map(body, mesh=mesh, in_specs=in_specs, out_specs=(P("rows", None), P()), check_vma=False)
```
